128 devices in a mesh: gx: 16 (over x_lo, y, core), gy: 8 (over z, x_hi).
Axes of the slice: x: 4 (x_hi: 2, x_lo: 2; x = x_hi * 2 + x_lo), y: 4, z: 4, core: 2. Of those that a mesh axis runs over, the one named last changes fastest.
Arguments:
- collocation: bfloat16 [3072, 16384], P(None, 'gx'), may hold values from -6 to 6
- density: bfloat16 [3072, 3072], P('gy'), may hold values from -0.109375 to 0.109375
- kernel: bfloat16 [16384, 16, 8, 128], P('gx', None, 'gy'), may hold values from -6.67572e-06 to 6.67572e-06
Outputs:
- exchange: float32 [3072, 3072], P('gx', 'gy')
The draws below stay inside these ranges and needn't reach their ends.
All inputs are finite; a program needn't handle non-finite values.
Results may differ from the reference program's by a relative error of at most 0.008.
Values may be sent and summed in bfloat16 or wider, within the bound.
No kernel may reach another device: no remote copies, remote signals or barrier semaphores. Data moves between devices by JAX's collectives and lax.ppermute only.
A program may use at most 448 MiB of HBM per device.

```python
import jax
import jax.numpy as jnp
from jax import lax

NBF = 3072
NPTS = 16384
CYCLE_LEN = 16
COL_GROUPS = 8
PIECE = 128
N_GX = 16


def block_levels(stream_key, shape, pieces, smallest, high):
    factor_of, own = 1.0, jax.random.fold_in(stream_key, 6)
    for dim, blocks in pieces:
        steps = jnp.exp(jax.random.uniform(jax.random.fold_in(own, dim), (blocks,), jnp.float32, smallest / len(pieces), high / len(pieces)))
        factor_of = factor_of * jnp.repeat(steps, shape[dim] // blocks).reshape([-1 if axis == dim else 1 for axis in range(len(shape))])
    return factor_of


def noise(rng, shape, deviation, limit, cuts=(), held_as=jnp.bfloat16):
    values = deviation * jax.random.normal(rng, shape, jnp.float32)
    if cuts:
        values = values * block_levels(rng, shape, cuts, -0.22, 0.18)
    return jnp.clip(values, -limit, limit).astype(held_as)


def setup_inputs(seed: int = 0) -> dict:
    key_list = jax.random.split(jax.random.key(seed), 4)
    collocation = noise(key_list[0], (NBF, NPTS), 1.0, 6.0, ((1, 16),))
    density = noise(key_list[1], (NBF, NBF), NBF ** -0.5, 0.109375, ((0, 8),))
    kernel = noise(key_list[2], (NPTS, CYCLE_LEN, COL_GROUPS, PIECE), (NPTS * NPTS * NBF) ** -0.5, 6.67572021484375e-06, ((0, 16), (2, 8)))
    return {"collocation": collocation, "density": density, "kernel": kernel}


def reference(collocation, density, kernel):
    dense = jnp.dot(density, collocation, preferred_element_type=jnp.float32).astype(jnp.bfloat16)
    flat_kernel = kernel.reshape(NPTS, NPTS)
    block_len = NPTS // N_GX

    def scan_step(running, position):
        offset = (position * block_len).astype(jnp.int32)
        dense_rows = lax.dynamic_slice_in_dim(dense, offset, block_len, 1)
        colloc_rows = lax.dynamic_slice_in_dim(collocation, offset, block_len, 1)
        coefficients = lax.dynamic_slice_in_dim(flat_kernel, offset, block_len, 0)
        products = jnp.dot(dense_rows.T, collocation, preferred_element_type=jnp.float32)
        weighted = (coefficients.astype(jnp.float32) * products).astype(jnp.bfloat16)
        contracted = jnp.dot(weighted, collocation.T, preferred_element_type=jnp.float32).astype(jnp.bfloat16)
        return running + jnp.dot(colloc_rows, contracted, preferred_element_type=jnp.float32), None

    running, unused = lax.scan(scan_step, jnp.zeros((NBF, NBF), jnp.float32), jnp.arange(N_GX, dtype=jnp.int32))
    return running
```

```python
import functools

import jax
import jax.numpy as jnp
from jax import lax
from jax.experimental import pallas as pl
from jax.experimental.pallas import tpu as pltpu
from jax.sharding import PartitionSpec as P


BF = jnp.bfloat16
F32 = jnp.float32
ANY = pl.BlockSpec(memory_space=pl.ANY)
SMEM = pl.BlockSpec(memory_space=pltpu.SMEM)
VMEM_LIMIT = 60 * 1024 * 1024
AT_Z, AT_ROWS, AT_X = 25, 28, 44


def gx_pairs(f):
    out = []
    for a in range(2):
        for b in range(4):
            for c in range(2):
                ta, tb, tc = f(a, b, c)
                out.append(((a * 4 + b) * 2 + c, (ta * 4 + tb % 4) * 2 + tc))
    return out


def gy_pairs(f):
    out = []
    for z in range(4):
        for h in range(2):
            tz, th = f(z, h)
            out.append((z * 2 + h, (tz % 4) * 2 + th))
    return out


def both_pairs(f):
    out = []
    for g in range(16):
        for z in range(4):
            for h in range(2):
                tz, th = f(g % 2, z, h)
                out.append((g * 8 + z * 2 + h, g * 8 + (tz % 4) * 2 + th))
    return out


CORE = gx_pairs(lambda a, b, c: (a, b, 1 - c))
XLO = gx_pairs(lambda a, b, c: (1 - a, b, c))
YSPLIT = gx_pairs(lambda a, b, c: (a, b + 1 if c == 0 else b - 1, c))
ZSPLIT = both_pairs(lambda c, z, h: (z + 1 if c == 0 else z - 1, h))
XHI = gy_pairs(lambda z, h: (z, 1 - h))
ZUP = gy_pairs(lambda z, h: (z + 1, h))
ZDOWN = gy_pairs(lambda z, h: (z - 1, h))


def gx_perm(x, pairs):
    return lax.ppermute(x, "gx", pairs)


def gy_perm(x, pairs):
    return lax.ppermute(x, "gy", pairs)


def both_perm(x, pairs):
    return lax.ppermute(x, ("gx", "gy"), pairs)


def after(x, *others):
    return lax.optimization_barrier((x, *others))[0]


def lanes(ref, first, n, rows=slice(None)):
    return jnp.concatenate([ref[first + i, rows, :] for i in range(n)], axis=1)


def ahead(q, n, limit, fetch):
    for k in range(n, limit):
        pl.when(q + n == k)(functools.partial(fetch, k))


def early_kernel(n_d, n_c, mu, tab, *refs):
    d_refs, c_refs, o_ref = refs[:n_d], refs[n_d : n_d + n_c], refs[n_d + n_c]
    d_s, c_s, o_s, d_sem, c_sem, o_sem = refs[n_d + n_c + 1 :]

    def c_copy(ref, p, j, rows):
        return pltpu.make_async_copy(
            ref.at[pl.ds(rows, mu), :], c_s.at[p, pl.ds(j * mu, mu), :], c_sem.at[p, j]
        )

    def o_copy(q):
        return pltpu.make_async_copy(o_s.at[q], o_ref.at[q], o_sem.at[q])

    def fetch(q):
        for p in range(4 * q, 4 * q + 4):
            for j in range(n_d):
                c_copy(c_refs[p], p, j, pl.multiple_of(tab[j] * mu, mu)).start()

    for j in range(n_d):
        pltpu.make_async_copy(d_refs[j], d_s.at[j], d_sem.at[j]).start()
    fetch(0)
    for j in range(n_d):
        pltpu.make_async_copy(d_refs[j], d_s.at[j], d_sem.at[j]).wait()
    fetch(1)

    def tile(q, carry):
        for i in range(4):
            for j in range(n_d):
                c_copy(c_refs[0], 4 * q + i, j, 0).wait()
        ahead(q, 2, n_c // 4, fetch)
        for h in range(2):
            o_s[2 * q + h] = jnp.dot(
                lanes(d_s, 0, n_d), lanes(c_s, 4 * q + 2 * h, 2), preferred_element_type=F32
            ).astype(BF)
        o_copy(2 * q).start()
        o_copy(2 * q + 1).start()
        return carry

    lax.fori_loop(0, n_c // 4, tile, 0)
    for q in range(n_c // 4):
        o_copy(2 * q).wait()
        o_copy(2 * q + 1).wait()


def early(tab, blocks, pieces, mu):
    n_d, n_c = len(blocks), len(pieces)
    panel = blocks[0].shape[0]
    return pl.pallas_call(
        functools.partial(early_kernel, n_d, n_c, mu),
        out_shape=jax.ShapeDtypeStruct((n_c // 2, panel, 256), BF),
        in_specs=[SMEM] + [ANY] * (n_d + n_c),
        out_specs=ANY,
        scratch_shapes=[
            pltpu.VMEM((n_d, panel, mu), BF),
            pltpu.VMEM((n_c, n_d * mu, 128), BF),
            pltpu.VMEM((n_c // 2, panel, 256), BF),
            pltpu.SemaphoreType.DMA((n_d,)),
            pltpu.SemaphoreType.DMA((n_c, n_d)),
            pltpu.SemaphoreType.DMA((n_c // 2,)),
        ],
        compiler_params=pltpu.CompilerParams(vmem_limit_bytes=VMEM_LIMIT),
        cost_estimate=pl.CostEstimate(
            flops=2 * panel * n_c * 128 * n_d * mu, bytes_accessed=24 << 20, transcendentals=0
        ),
        name="early",
    )(tab, *blocks, *pieces)


def weigh_kernel(n_d, n_c, mu, first, tab, *refs):
    acc_ref, z_ref = refs[:2]
    d_refs, c_refs = refs[2 : 2 + n_d], refs[2 + n_d : 2 + n_d + n_c]
    outs = refs[2 + n_d + n_c : 7 + n_d + n_c]
    w_out, u_outs = outs[0], outs[1:]
    d_s, c_s, f_s, z_s, w_s, u_s, d_sem, c_sem, f_sem, z_sem, a_sem, o_sem, u_sem = refs[
        7 + n_d + n_c :
    ]
    width = 2 * mu
    tiles = n_c // 2

    def c_copy(ref, p, j, rows):
        return pltpu.make_async_copy(
            ref.at[pl.ds(rows, mu), :], c_s.at[p, pl.ds(j * mu, mu), :], c_sem.at[p, j]
        )

    def z_copy(p, k):
        return pltpu.make_async_copy(z_ref.at[k], z_s.at[p], z_sem.at[p])

    def acc_copy(q):
        return pltpu.make_async_copy(acc_ref.at[q], w_s.at[q], a_sem.at[q])

    def far_copy(p):
        rows = pl.multiple_of(tab[24] * width, width)
        return pltpu.make_async_copy(c_refs[p].at[pl.ds(rows, width), :], f_s.at[p], f_sem.at[p])

    def w_copy(q):
        return pltpu.make_async_copy(w_s.at[q], w_out.at[q], o_sem.at[q])

    for j in range(n_d):
        pltpu.make_async_copy(d_refs[j], d_s.at[j], d_sem.at[j]).start()

    def fetch(q):
        for p in (2 * q, 2 * q + 1):
            for j in range(n_d):
                c_copy(c_refs[p], p, j, pl.multiple_of(tab[first + j] * mu, mu)).start()
            z_copy(p, tab[8 + p]).start()
        acc_copy(q).start()

    def fetch_far(q):
        for p in (2 * q, 2 * q + 1):
            far_copy(p).start()

    for q in range(2):
        fetch(q)
    for j in range(n_d):
        pltpu.make_async_copy(d_refs[j], d_s.at[j], d_sem.at[j]).wait()
    fetch(2)

    def tile(q, carry):
        for i in range(2):
            for j in range(n_d):
                c_copy(c_refs[0], 2 * q + i, j, 0).wait()
            z_copy(2 * q + i, 0).wait()
        acc_copy(q).wait()
        ahead(q, 3, tiles, fetch)
        ahead(q, 0, tiles, fetch_far)
        product = jnp.dot(
            lanes(d_s, 0, n_d), lanes(c_s, 2 * q, 2), preferred_element_type=F32
        )
        product = product + w_s[q].astype(F32)
        w_s[q] = (lanes(z_s, 2 * q, 2).astype(F32) * product).astype(BF)
        w_copy(q).start()
        return carry

    lax.fori_loop(0, tiles, tile, 0)
    for p in range(n_c):
        far_copy(p).wait()

    quarter = u_s.shape[0] // 4

    def u_copy(i):
        return pltpu.make_async_copy(
            u_s.at[pl.ds(i * quarter, quarter), :], u_outs[i], u_sem.at[i]
        )

    for i in range(4):
        part = pl.ds(i * quarter, quarter)
        u_s[part, :] = lax.dot_general(
            lanes(w_s, 0, tiles, part), lanes(f_s, 0, n_c), (((1,), (1,)), ((), ())),
            preferred_element_type=F32,
        ).astype(BF)
        u_copy(i).start()
    for q in range(tiles):
        w_copy(q).wait()
    for i in range(4):
        u_copy(i).wait()


def weigh(tab, acc, tiles, blocks, pieces, mu, first):
    n_d, n_c = len(blocks), len(pieces)
    panel = blocks[0].shape[0]
    part = jax.ShapeDtypeStruct((panel // 4, 2 * mu), BF)
    return pl.pallas_call(
        functools.partial(weigh_kernel, n_d, n_c, mu, first),
        out_shape=(jax.ShapeDtypeStruct((n_c // 2, panel, 256), BF), part, part, part, part),
        in_specs=[SMEM] + [ANY] * (n_d + n_c + 2),
        out_specs=(ANY,) * 5,
        scratch_shapes=[
            pltpu.VMEM((n_d, panel, mu), BF),
            pltpu.VMEM((n_c, n_d * mu, 128), BF),
            pltpu.VMEM((n_c, 2 * mu, 128), BF),
            pltpu.VMEM((n_c, panel, 128), BF),
            pltpu.VMEM((n_c // 2, panel, 256), BF),
            pltpu.VMEM((panel, 2 * mu), BF),
            pltpu.SemaphoreType.DMA((n_d,)),
            pltpu.SemaphoreType.DMA((n_c, n_d)),
            pltpu.SemaphoreType.DMA((n_c,)),
            pltpu.SemaphoreType.DMA((n_c,)),
            pltpu.SemaphoreType.DMA((n_c // 2,)),
            pltpu.SemaphoreType.DMA((n_c // 2,)),
            pltpu.SemaphoreType.DMA((4,)),
        ],
        compiler_params=pltpu.CompilerParams(vmem_limit_bytes=VMEM_LIMIT),
        cost_estimate=pl.CostEstimate(
            flops=2 * panel * n_c * 128 * (n_d + 2) * mu, bytes_accessed=24 << 20, transcendentals=0
        ),
        name="weigh",
    )(tab, acc, tiles, *blocks, *pieces)


def spread_kernel(n_c, mu, at, n_out, tab, *refs):
    w_ref, c_refs = refs[0], refs[1 : 1 + n_c]
    o_ref = refs[1 + n_c]
    w_s, c_s, u_s, w_sem, c_sem, o_sem = refs[2 + n_c :]
    width = 2 * mu

    def c_copy(ref, p, i, rows):
        return pltpu.make_async_copy(
            ref.at[pl.ds(rows, width), :], c_s.at[i, p], c_sem.at[i, p]
        )

    w_copy = pltpu.make_async_copy(w_ref, w_s, w_sem)
    w_copy.start()
    for i in range(n_out):
        for p in range(n_c):
            c_copy(c_refs[p], p, i, pl.multiple_of(tab[at + i] * width, width)).start()
        if i == 0:
            w_copy.wait()

    def block(i, carry):
        for p in range(n_c):
            c_copy(c_refs[0], p, i, 0).wait()
        u_s[i] = lax.dot_general(
            lanes(w_s, 0, n_c // 2), lanes(c_s.at[i], 0, n_c), (((1,), (1,)), ((), ())),
            preferred_element_type=F32,
        ).astype(BF)
        pltpu.make_async_copy(u_s.at[i], o_ref.at[i], o_sem.at[i]).start()
        return carry

    lax.fori_loop(0, n_out, block, 0)
    for i in range(n_out):
        pltpu.make_async_copy(u_s.at[i], o_ref.at[i], o_sem.at[i]).wait()


def spread(tab, weighted, pieces, mu, at, n_out):
    n_c = len(pieces)
    panel = weighted.shape[1]
    width = 2 * mu
    return pl.pallas_call(
        functools.partial(spread_kernel, n_c, mu, at, n_out),
        out_shape=jax.ShapeDtypeStruct((n_out, panel, width), BF),
        in_specs=[SMEM] + [ANY] * (1 + n_c),
        out_specs=ANY,
        scratch_shapes=[
            pltpu.VMEM(weighted.shape, BF),
            pltpu.VMEM((n_out, n_c, width, 128), BF),
            pltpu.VMEM((n_out, panel, width), BF),
            pltpu.SemaphoreType.DMA,
            pltpu.SemaphoreType.DMA((n_out, n_c)),
            pltpu.SemaphoreType.DMA((n_out,)),
        ],
        compiler_params=pltpu.CompilerParams(vmem_limit_bytes=VMEM_LIMIT),
        cost_estimate=pl.CostEstimate(
            flops=2 * panel * n_c * 128 * n_out * width, bytes_accessed=20 << 20, transcendentals=0
        ),
    )(tab, weighted, *pieces)


VM = pl.BlockSpec(memory_space=pltpu.VMEM)


def merge_kernel(i, half, first, base_ref, got_ref, out_ref, buf, sem):
    rows, quarter = buf.shape[0], got_ref.shape[0]
    copy = pltpu.make_async_copy(base_ref.at[i, pl.ds(half * rows, rows), :], buf, sem)
    copy.start()
    copy.wait()
    with_got = slice(0, quarter) if first else slice(quarter, 2 * quarter)
    without = slice(quarter, 2 * quarter) if first else slice(0, quarter)
    out_ref[without, :] = buf[without, :]
    out_ref[with_got, :] = (buf[with_got, :].astype(F32) + got_ref[...].astype(F32)).astype(BF)


def merge(base, got, i, half, first):
    rows, width = base.shape[1] // 2, base.shape[2]
    return pl.pallas_call(
        functools.partial(merge_kernel, i, half, first),
        in_specs=[ANY, VM],
        out_specs=VM,
        out_shape=jax.ShapeDtypeStruct((rows, width), BF),
        scratch_shapes=[pltpu.VMEM((rows, width), BF), pltpu.SemaphoreType.DMA],
        compiler_params=pltpu.CompilerParams(vmem_limit_bytes=8 << 20),
        cost_estimate=pl.CostEstimate(
            flops=rows * width * 64, bytes_accessed=rows * width * 4, transcendentals=0
        ),
    )(base, got)


def total_kernel(half, mu, tab, base_ref, below_ref, above_ref, sent_ref, kept_ref):
    rows = sent_ref.shape[0]
    part = slice(half * rows, (half + 1) * rows)
    for i, out in ((0, sent_ref), (1, kept_ref)):
        cols = pl.ds(pl.multiple_of(tab[AT_X + i] * mu, mu), mu)
        out[...] = (
            base_ref[0, part, cols].astype(F32)
            + below_ref[:, cols].astype(F32)
            + above_ref[:, cols].astype(F32)
        ).astype(out.dtype)


def totals(tab, base, below, above, half, mu):
    rows, width = below.shape
    return pl.pallas_call(
        functools.partial(total_kernel, half, mu),
        in_specs=[SMEM, VM, VM, VM],
        out_specs=(VM, VM),
        out_shape=(
            jax.ShapeDtypeStruct((rows, mu), BF),
            jax.ShapeDtypeStruct((rows, mu), F32),
        ),
        compiler_params=pltpu.CompilerParams(vmem_limit_bytes=8 << 20),
        cost_estimate=pl.CostEstimate(
            flops=rows * width * 64, bytes_accessed=rows * width * 8, transcendentals=0
        ),
    )(tab, base, below, above)


def pick_kernel(tab, c_ref, keep_ref, send_ref, buf, in_sem, out_sem):
    n, rows = 8, buf.shape[1] // 8

    def get(i, j):
        start = pl.multiple_of(tab[AT_ROWS + i * n + j] * rows, rows)
        return pltpu.make_async_copy(
            c_ref.at[pl.ds(start, rows), :], buf.at[i, pl.ds(j * rows, rows), :], in_sem.at[i, j]
        )

    for i in range(2):
        for j in range(n):
            get(i, j).start()
    for i, out in ((0, send_ref), (1, keep_ref)):
        for j in range(n):
            get(i, j).wait()
        pltpu.make_async_copy(buf.at[i], out, out_sem.at[i]).start()
    for i, out in ((0, send_ref), (1, keep_ref)):
        pltpu.make_async_copy(buf.at[i], out, out_sem.at[i]).wait()


def pick(tab, collocation):
    nbf, panel = collocation.shape
    block = jax.ShapeDtypeStruct((nbf // 2, panel), BF)
    return pl.pallas_call(
        pick_kernel,
        out_shape=(block, block),
        in_specs=[SMEM, ANY],
        out_specs=(ANY, ANY),
        scratch_shapes=[
            pltpu.VMEM((2, nbf // 2, panel), BF),
            pltpu.SemaphoreType.DMA((2, 8)),
            pltpu.SemaphoreType.DMA((2,)),
        ],
        cost_estimate=pl.CostEstimate(
            flops=1 << 30, bytes_accessed=4 * nbf * panel, transcendentals=0
        ),
        name="pick",
    )(tab, collocation)


def first_kernel(own_ref, par_ref, r_ref, rp_ref, o_ref):
    depth = r_ref.shape[0]
    o_ref[...] = jnp.dot(
        own_ref[:, :depth], r_ref[...], preferred_element_type=F32
    ) + jnp.dot(par_ref[:, :depth], rp_ref[...], preferred_element_type=F32)


def last_kernel(own_ref, par_ref, r_ref, rp_ref, acc_ref, *outs):
    rows, depth = outs[0].shape[0], r_ref.shape[0]
    for j, out in enumerate(outs):
        part = slice(j * rows, (j + 1) * rows)
        out[...] = (
            acc_ref[part, :]
            + jnp.dot(own_ref[part, depth:], r_ref[...], preferred_element_type=F32)
            + jnp.dot(par_ref[part, depth:], rp_ref[...], preferred_element_type=F32)
        ).astype(out.dtype)


def k_rows(own, par, red, red_par, acc=None):
    n, depth = own.shape[0], red.shape[0]
    mu = red.shape[1]
    cost = pl.CostEstimate(flops=4 * n * depth * mu, bytes_accessed=6 << 20, transcendentals=0)
    params = pltpu.CompilerParams(vmem_limit_bytes=16 << 20)
    if acc is None:
        return pl.pallas_call(
            first_kernel, in_specs=[VM] * 4, out_specs=VM, compiler_params=params,
            out_shape=jax.ShapeDtypeStruct((n, mu), F32), cost_estimate=cost, name="k_first",
        )(own, par, red, red_par)
    return pl.pallas_call(
        last_kernel, in_specs=[VM] * 5, out_specs=(VM,) * 8, compiler_params=params,
        out_shape=tuple(
            jax.ShapeDtypeStruct((n // 8, mu), F32 if j == 0 else BF) for j in range(8)
        ),
        cost_estimate=cost, name="k_last",
    )(own, par, red, red_par, acc)


def exchange(collocation, density, kernel):
    w = kernel.shape[3]
    gx = lax.axis_index("gx")
    gy = lax.axis_index("gy")
    core, y, xlo = gx & 1, (gx >> 1) & 3, gx >> 3
    z, xhi = gy >> 1, gy & 1
    sign = 1 - 2 * core
    mu = density.shape[0]

    own_piece = lax.dynamic_slice_in_dim(collocation, gy * w, w, 1)
    own_t = lax.dot_general(
        collocation, density, (((0,), (1,)), ((), ())), preferred_element_type=F32
    ).astype(BF)

    near = gx_perm(own_piece, YSPLIT)
    other = gx_perm(own_piece, CORE)
    piece_x = gx_perm(own_piece, XLO)
    near_other = gx_perm(other, YSPLIT)
    d_near = both_perm(own_t, ZSPLIT)
    d_other = gx_perm(own_t, CORE)
    d_near_other = both_perm(d_other, ZSPLIT)
    far = gx_perm(near, YSPLIT)
    own_x = gy_perm(own_t, XHI)
    d_far = both_perm(d_near, ZSPLIT)
    px = piece_x
    other_x = gx_perm(px, CORE)
    near_x = gx_perm(px, YSPLIT)
    near_other_x = gx_perm(other_x, YSPLIT)
    dx = own_x
    d_other_x = gx_perm(dx, CORE)
    d_near_x = both_perm(dx, ZSPLIT)
    d_near_other_x = both_perm(d_other_x, ZSPLIT)
    far_x = gx_perm(near_x, YSPLIT)
    d_far_x = both_perm(d_near_x, ZSPLIT)
    pieces = [
        own_piece, other, near, near_other,
        gx_perm(near_other, CORE), gx_perm(near, CORE),
        far, gx_perm(far, CORE),
        piece_x, other_x, near_x, near_other_x,
        gx_perm(near_other_x, CORE), gx_perm(near_x, CORE),
        far_x, gx_perm(far_x, CORE),
    ]
    blocks = [
        own_t, d_near, gx_perm(d_near_other, CORE), d_far,
        own_x, d_near_x, gx_perm(d_near_other_x, CORE), d_far_x,
    ]
    k_tab = []
    for xl in (xlo, 1 - xlo):
        for yy in (y, y - sign, y + sign, y + 2):
            for cc in (core, 1 - core):
                k_tab.append((xl * 4 + (yy & 3)) * 2 + cc)
    m_tab = []
    for h in (xhi, 1 - xhi):
        for zz in (z, z - sign, z + sign, z + 2):
            m_tab.append((zz & 3) * 2 + h)
    m_tab = [m_tab[j] for j in (0, 1, 2, 3, 4, 5, 7, 6)]

    tiles = jnp.transpose(after(kernel, near)[:, :, 0, :], (1, 0, 2))

    hops = [(dx, dy) for dx in (0, 1) for dy in range(4)]
    chips = [((xlo ^ dx) * 4 + ((y + dy) & 3)) * 2 for dx, dy in hops]
    tab = jnp.stack(
        m_tab + k_tab + [(z + 2) & 3, (z + 1) & 3, (z + 3) & 3, z]
        + [c + 1 - core for c in chips] + [c + core for c in chips] + [1 - xhi, xhi]
    ).astype(jnp.int32)
    blocks = [blocks[j] for j in (0, 1, 2, 3, 4, 5, 7, 6)]
    acc = early(tab, blocks[:6], pieces, mu)
    weighted, a1, a2, b1, b2 = weigh(tab, acc, tiles, blocks[6:], pieces, mu, 6)

    a1 = gy_perm(a1, ZUP)
    a2 = gy_perm(a2, ZDOWN)
    b1 = gy_perm(b1, ZUP)
    b2 = gy_perm(b2, ZDOWN)
    near_u = spread(tab, weighted, pieces, mu, AT_Z, 2)
    zero = spread(tab, weighted, pieces, mu, AT_Z + 2, 1)
    up_a = gy_perm(merge(near_u, a1, 0, 0, True), ZUP)
    down_a = gy_perm(merge(near_u, a2, 1, 0, False), ZDOWN)
    up_b = gy_perm(merge(near_u, b1, 0, 1, True), ZUP)
    down_b = gy_perm(merge(near_u, b2, 1, 1, False), ZDOWN)

    c_own, c_send = pick(tab, after(collocation, far))
    c_par = gx_perm(c_send, CORE)

    def finish(half, below, above):
        sent, kept = totals(tab, zero, below, above, half, mu)
        red = (kept + gy_perm(sent, XHI).astype(F32)).astype(BF)
        return red, gx_perm(red, CORE)

    part = k_rows(c_own, c_par, *finish(0, up_a, down_a))
    rows = k_rows(c_own, c_par, *finish(1, up_b, down_b), part)
    total = rows[0]
    for i in (6, 5, 7, 2, 1, 3, 4):
        dx, dy = hops[i]
        pairs = gx_pairs(lambda a, b, c, dx=dx, dy=dy: (a ^ dx, b + dy, c))
        total = total + gx_perm(rows[i], pairs).astype(F32)
    return total


def solution(mesh):
    return jax.shard_map(
        exchange,
        mesh=mesh,
        in_specs=(P(None, "gx"), P("gy", None), P("gx", None, "gy", None)),
        out_specs=P("gx", "gy"),
        check_vma=False,
    )
```

```python
import functools

import jax
import jax.numpy as jnp
from jax import lax
from jax.experimental import pallas as pl
from jax.experimental.pallas import tpu as pltpu
from jax.sharding import PartitionSpec as P


BF = jnp.bfloat16
F32 = jnp.float32
ANY = pl.BlockSpec(memory_space=pl.ANY)
SMEM = pl.BlockSpec(memory_space=pltpu.SMEM)
VM = pl.BlockSpec(memory_space=pltpu.VMEM)
AT_OWN, AT_OTHER, AT_ROWS = 24, 28, 32


def gx_pairs(f):
    out = []
    for a in range(2):
        for b in range(4):
            for c in range(2):
                ta, tb, tc = f(a, b, c)
                out.append(((a * 4 + b) * 2 + c, (ta * 4 + tb % 4) * 2 + tc))
    return out


def gy_pairs(f):
    out = []
    for z in range(4):
        for h in range(2):
            tz, th = f(z, h)
            out.append((z * 2 + h, (tz % 4) * 2 + th))
    return out


def both_pairs(f):
    out = []
    for g in range(16):
        for z in range(4):
            for h in range(2):
                tz, th = f(g % 2, z, h)
                out.append((g * 8 + z * 2 + h, g * 8 + (tz % 4) * 2 + th))
    return out


CORE = gx_pairs(lambda a, b, c: (a, b, 1 - c))
XLO = gx_pairs(lambda a, b, c: (1 - a, b, c))
YSPLIT = gx_pairs(lambda a, b, c: (a, b + 1 if c == 0 else b - 1, c))
ZSPLIT = both_pairs(lambda c, z, h: (z + 1 if c == 0 else z - 1, h))
XHI = gy_pairs(lambda z, h: (z, 1 - h))
ZUP = gy_pairs(lambda z, h: (z + 1, h))
ZDOWN = gy_pairs(lambda z, h: (z - 1, h))


def gx_perm(x, pairs):
    return lax.ppermute(x, "gx", pairs)


def gy_perm(x, pairs):
    return lax.ppermute(x, "gy", pairs)


def both_perm(x, pairs):
    return lax.ppermute(x, ("gx", "gy"), pairs)


def after(x, *others):
    return lax.optimization_barrier((x, *others))[0]


def lanes(ref, first, n, rows=slice(None)):
    return jnp.concatenate([ref[first + i, rows, :] for i in range(n)], axis=1)


def ahead(q, n, limit, fetch):
    for k in range(n, limit):
        pl.when(q + n == k)(functools.partial(fetch, k))


def early_kernel(n_d, n_c, mu, tab, *refs):
    d_refs, c_refs, o_ref = refs[:n_d], refs[n_d : n_d + n_c], refs[n_d + n_c]
    d_s, c_s, o_s, d_sem, c_sem, o_sem = refs[n_d + n_c + 1 :]

    def c_copy(ref, p, j, rows):
        return pltpu.make_async_copy(
            ref.at[pl.ds(rows, mu), :], c_s.at[p, pl.ds(j * mu, mu), :], c_sem.at[p, j]
        )

    def o_copy(q):
        return pltpu.make_async_copy(o_s.at[q], o_ref.at[q], o_sem.at[q])

    def fetch(q):
        for p in range(4 * q, 4 * q + 4):
            for j in range(n_d):
                c_copy(c_refs[p], p, j, pl.multiple_of(tab[j] * mu, mu)).start()

    for j in range(n_d):
        pltpu.make_async_copy(d_refs[j], d_s.at[j], d_sem.at[j]).start()
    fetch(0)
    for j in range(n_d):
        pltpu.make_async_copy(d_refs[j], d_s.at[j], d_sem.at[j]).wait()
    fetch(1)

    def tile(q, carry):
        for i in range(4):
            for j in range(n_d):
                c_copy(c_refs[0], 4 * q + i, j, 0).wait()
        ahead(q, 2, n_c // 4, fetch)
        for h in range(2):
            o_s[2 * q + h] = jnp.dot(
                lanes(d_s, 0, n_d), lanes(c_s, 4 * q + 2 * h, 2), preferred_element_type=F32
            ).astype(BF)
        o_copy(2 * q).start()
        o_copy(2 * q + 1).start()
        return carry

    lax.fori_loop(0, n_c // 4, tile, 0)
    for q in range(n_c // 4):
        o_copy(2 * q).wait()
        o_copy(2 * q + 1).wait()


def early(tab, blocks, pieces, mu):
    n_d, n_c = len(blocks), len(pieces)
    panel = blocks[0].shape[0]
    return pl.pallas_call(
        functools.partial(early_kernel, n_d, n_c, mu),
        out_shape=jax.ShapeDtypeStruct((n_c // 2, panel, 256), BF),
        in_specs=[SMEM] + [ANY] * (n_d + n_c),
        out_specs=ANY,
        scratch_shapes=[
            pltpu.VMEM((n_d, panel, mu), BF),
            pltpu.VMEM((n_c, n_d * mu, 128), BF),
            pltpu.VMEM((n_c // 2, panel, 256), BF),
            pltpu.SemaphoreType.DMA((n_d,)),
            pltpu.SemaphoreType.DMA((n_c, n_d)),
            pltpu.SemaphoreType.DMA((n_c // 2,)),
        ],
        compiler_params=pltpu.CompilerParams(vmem_limit_bytes=60 << 20),
        cost_estimate=pl.CostEstimate(
            flops=2 * panel * n_c * 128 * n_d * mu, bytes_accessed=24 << 20, transcendentals=0
        ),
        name="early",
    )(tab, *blocks, *pieces)


def u_parts(w_ref, c_s, first_row, mu, outs):
    u = lax.dot_general(
        lanes(w_ref, 0, w_ref.shape[0]),
        lanes(c_s, 0, c_s.shape[0], slice(first_row, first_row + 2 * mu)),
        (((1,), (1,)), ((), ())), preferred_element_type=F32,
    ).astype(BF)
    half = u.shape[0] // 2
    a_refs, own_ref, other_ref = outs[:-2], outs[-2], outs[-1]
    rows = half // len(a_refs)
    for i, ref in enumerate(a_refs):
        ref[...] = u[i * rows : (i + 1) * rows]
    own_ref[...] = u[half:, :mu]
    other_ref[...] = u[half:, mu:]


def u_shapes(half, mu, parts):
    a = (jax.ShapeDtypeStruct((half // parts, 2 * mu), BF),) * parts
    return a + (jax.ShapeDtypeStruct((half, mu), BF),) * 2


def weigh_kernel(n_d, n_c, mu, first, tab, *refs):
    acc_ref, z_ref = refs[:2]
    d_refs, c_refs = refs[2 : 2 + n_d], refs[2 + n_d : 2 + n_d + n_c]
    outs = refs[2 + n_d + n_c : 10 + n_d + n_c]
    d_s, c_s, f_s, z_s, w_s, d_sem, c_sem, f_sem, z_sem, a_sem, o_sem = refs[10 + n_d + n_c :]
    tiles = n_c // 2

    def c_copy(ref, p, j, rows):
        return pltpu.make_async_copy(
            ref.at[pl.ds(rows, mu), :], c_s.at[p, pl.ds(j * mu, mu), :], c_sem.at[p, j]
        )

    def z_copy(p, k):
        return pltpu.make_async_copy(z_ref.at[k], z_s.at[p], z_sem.at[p])

    def acc_copy(q):
        return pltpu.make_async_copy(acc_ref.at[q], w_s.at[q], a_sem.at[q])

    def far_copy(p, i):
        place = tab[(AT_OWN, AT_OTHER)[i % 2] + i // 2]
        return pltpu.make_async_copy(
            c_refs[p].at[pl.ds(pl.multiple_of(place * mu, mu), mu), :],
            f_s.at[p, pl.ds(i * mu, mu), :], f_sem.at[p, i],
        )

    def w_copy(q):
        return pltpu.make_async_copy(w_s.at[q], outs[0].at[q], o_sem.at[q])

    def fetch(q):
        for p in (2 * q, 2 * q + 1):
            for j in range(n_d):
                c_copy(c_refs[p], p, j, pl.multiple_of(tab[first + j] * mu, mu)).start()
            z_copy(p, tab[8 + p]).start()
        acc_copy(q).start()

    def fetch_far(q):
        for p in (2 * q, 2 * q + 1):
            for i in range(4):
                far_copy(p, i).start()

    for j in range(n_d):
        pltpu.make_async_copy(d_refs[j], d_s.at[j], d_sem.at[j]).start()
    for q in range(2):
        fetch(q)
    for j in range(n_d):
        pltpu.make_async_copy(d_refs[j], d_s.at[j], d_sem.at[j]).wait()
    fetch(2)

    def tile(q, carry):
        for i in range(2):
            for j in range(n_d):
                c_copy(c_refs[0], 2 * q + i, j, 0).wait()
            z_copy(2 * q + i, 0).wait()
        acc_copy(q).wait()
        ahead(q, 3, tiles, fetch)
        ahead(q, 0, tiles, fetch_far)
        product = jnp.dot(
            lanes(d_s, 0, n_d), lanes(c_s, 2 * q, 2), preferred_element_type=F32
        )
        product = product + w_s[q].astype(F32)
        w_s[q] = (lanes(z_s, 2 * q, 2).astype(F32) * product).astype(BF)
        w_copy(q).start()
        return carry

    lax.fori_loop(0, tiles, tile, 0)
    for p in range(n_c):
        for i in range(4):
            far_copy(p, i).wait()
    u_parts(w_s, f_s, 0, mu, outs[1:5])
    u_parts(w_s, f_s, 2 * mu, mu, outs[5:8])
    for q in range(tiles):
        w_copy(q).wait()


def weigh(tab, acc, tiles, blocks, pieces, mu, first):
    n_d, n_c = len(blocks), len(pieces)
    panel = blocks[0].shape[0]
    half = panel // 2
    return pl.pallas_call(
        functools.partial(weigh_kernel, n_d, n_c, mu, first),
        out_shape=(jax.ShapeDtypeStruct((n_c // 2, panel, 256), BF),)
        + u_shapes(half, mu, 2) + u_shapes(half, mu, 1),
        in_specs=[SMEM] + [ANY] * (n_d + n_c + 2),
        out_specs=(ANY,) + (VM,) * 7,
        scratch_shapes=[
            pltpu.VMEM((n_d, panel, mu), BF),
            pltpu.VMEM((n_c, n_d * mu, 128), BF),
            pltpu.VMEM((n_c, 4 * mu, 128), BF),
            pltpu.VMEM((n_c, panel, 128), BF),
            pltpu.VMEM((n_c // 2, panel, 256), BF),
            pltpu.SemaphoreType.DMA((n_d,)),
            pltpu.SemaphoreType.DMA((n_c, n_d)),
            pltpu.SemaphoreType.DMA((n_c, 4)),
            pltpu.SemaphoreType.DMA((n_c,)),
            pltpu.SemaphoreType.DMA((n_c // 2,)),
            pltpu.SemaphoreType.DMA((n_c // 2,)),
        ],
        compiler_params=pltpu.CompilerParams(vmem_limit_bytes=52 << 20),
        cost_estimate=pl.CostEstimate(
            flops=2 * panel * n_c * 128 * (n_d + 4) * mu, bytes_accessed=24 << 20, transcendentals=0
        ),
        name="weigh",
    )(tab, acc, tiles, *blocks, *pieces)


def spread_kernel(n_c, mu, at, tab, *refs):
    w_ref, c_refs = refs[0], refs[1 : 1 + n_c]
    outs, (w_s, c_s, w_sem, c_sem) = refs[1 + n_c : -4], refs[-4:]

    def c_copy(p, j):
        place = tab[(AT_OWN, AT_OTHER)[j] + at]
        return pltpu.make_async_copy(
            c_refs[p].at[pl.ds(pl.multiple_of(place * mu, mu), mu), :],
            c_s.at[p, pl.ds(j * mu, mu), :], c_sem.at[p, j],
        )

    w_copy = pltpu.make_async_copy(w_ref, w_s, w_sem)
    w_copy.start()
    for p in range(n_c):
        for j in range(2):
            c_copy(p, j).start()
    w_copy.wait()
    for p in range(n_c):
        for j in range(2):
            c_copy(p, j).wait()
    u_parts(w_s, c_s, 0, mu, outs)


def spread(tab, weighted, pieces, mu, at):
    n_c = len(pieces)
    half = weighted.shape[1] // 2
    return pl.pallas_call(
        functools.partial(spread_kernel, n_c, mu, at),
        out_shape=u_shapes(half, mu, 1),
        in_specs=[SMEM] + [ANY] * (n_c + 1),
        out_specs=(VM,) * 3,
        scratch_shapes=[
            pltpu.VMEM(weighted.shape, BF),
            pltpu.VMEM((n_c, 2 * mu, 128), BF),
            pltpu.SemaphoreType.DMA,
            pltpu.SemaphoreType.DMA((n_c, 2)),
        ],
        compiler_params=pltpu.CompilerParams(vmem_limit_bytes=52 << 20),
        cost_estimate=pl.CostEstimate(
            flops=4 * half * n_c * 128 * mu * 2, bytes_accessed=20 << 20, transcendentals=0
        ),
    )(tab, weighted, *pieces)


def small(kernel, out_shape, operands):
    many = isinstance(out_shape, tuple)
    return pl.pallas_call(
        kernel,
        in_specs=[VM] * len(operands),
        out_specs=(VM,) * len(out_shape) if many else VM,
        out_shape=out_shape,
        compiler_params=pltpu.CompilerParams(vmem_limit_bytes=12 << 20),
        cost_estimate=pl.CostEstimate(flops=1 << 26, bytes_accessed=4 << 20, transcendentals=0),
    )(*operands)


def pair_kernel(own_ref, got_ref, up_ref, down_ref):
    rows = up_ref.shape[0]
    for out, part in ((up_ref, slice(0, rows)), (down_ref, slice(rows, 2 * rows))):
        out[...] = (own_ref[part, :].astype(F32) + got_ref[part, :].astype(F32)).astype(BF)


def merge_a_kernel(i, base_ref, got_ref, out_ref):
    rows = got_ref.shape[0]
    there, rest = slice(i * rows, (i + 1) * rows), slice((1 - i) * rows, (2 - i) * rows)
    out_ref[rest, :] = base_ref[rest, :]
    out_ref[there, :] = (base_ref[there, :].astype(F32) + got_ref[...].astype(F32)).astype(BF)


def merge_b_kernel(i, base_ref, x_ref, got_ref, out_ref):
    rows = got_ref.shape[0]
    there, rest = slice(i * rows, (i + 1) * rows), slice((1 - i) * rows, (2 - i) * rows)
    out_ref[rest, :] = (base_ref[rest, :].astype(F32) + x_ref[rest, :].astype(F32)).astype(BF)
    out_ref[there, :] = (
        base_ref[there, :].astype(F32)
        + x_ref[there, :].astype(F32)
        + got_ref[...].astype(F32)
    ).astype(BF)


def total_a_kernel(base_ref, below_ref, above_ref, sent_ref, kept_ref):
    mu = sent_ref.shape[1]
    for out, cols in ((kept_ref, slice(0, mu)), (sent_ref, slice(mu, 2 * mu))):
        out[...] = (
            base_ref[:, cols].astype(F32)
            + below_ref[:, cols].astype(F32)
            + above_ref[:, cols].astype(F32)
        ).astype(out.dtype)


def total_b_kernel(base_ref, x_ref, below_ref, above_ref, out_ref):
    out_ref[...] = (
        base_ref[...].astype(F32)
        + x_ref[...].astype(F32)
        + below_ref[...].astype(F32)
        + above_ref[...].astype(F32)
    ).astype(BF)


def pick_kernel(tab, c_ref, keep_ref, send_ref, buf, in_sem, out_sem):
    n, rows = 8, buf.shape[1] // 8

    def get(i, j):
        start = pl.multiple_of(tab[AT_ROWS + i * n + j] * rows, rows)
        return pltpu.make_async_copy(
            c_ref.at[pl.ds(start, rows), :], buf.at[i, pl.ds(j * rows, rows), :], in_sem.at[i, j]
        )

    for i in range(2):
        for j in range(n):
            get(i, j).start()
    for i, out in ((0, send_ref), (1, keep_ref)):
        for j in range(n):
            get(i, j).wait()
        pltpu.make_async_copy(buf.at[i], out, out_sem.at[i]).start()
    for i, out in ((0, send_ref), (1, keep_ref)):
        pltpu.make_async_copy(buf.at[i], out, out_sem.at[i]).wait()


def pick(tab, collocation):
    nbf, panel = collocation.shape
    block = jax.ShapeDtypeStruct((nbf // 2, panel), BF)
    return pl.pallas_call(
        pick_kernel,
        out_shape=(block, block),
        in_specs=[SMEM, ANY],
        out_specs=(ANY, ANY),
        scratch_shapes=[
            pltpu.VMEM((2, nbf // 2, panel), BF),
            pltpu.SemaphoreType.DMA((2, 8)),
            pltpu.SemaphoreType.DMA((2,)),
        ],
        cost_estimate=pl.CostEstimate(
            flops=1 << 30, bytes_accessed=4 * nbf * panel, transcendentals=0
        ),
        name="pick",
    )(tab, collocation)


def first_kernel(own_ref, par_ref, r_ref, rp_ref, o_ref):
    depth = r_ref.shape[0]
    o_ref[...] = jnp.dot(
        own_ref[:, depth:], r_ref[...], preferred_element_type=F32
    ) + jnp.dot(par_ref[:, depth:], rp_ref[...], preferred_element_type=F32)


def last_kernel(own_ref, par_ref, r_ref, rp_ref, acc_ref, *outs):
    rows, depth = outs[0].shape[0], r_ref.shape[0]
    for j, out in enumerate(outs):
        part = slice(j * rows, (j + 1) * rows)
        out[...] = (
            acc_ref[part, :]
            + jnp.dot(own_ref[part, :depth], r_ref[...], preferred_element_type=F32)
            + jnp.dot(par_ref[part, :depth], rp_ref[...], preferred_element_type=F32)
        ).astype(out.dtype)


def k_rows(own, par, red, red_par, acc=None):
    n, depth = own.shape[0], red.shape[0]
    mu = red.shape[1]
    cost = pl.CostEstimate(flops=4 * n * depth * mu, bytes_accessed=6 << 20, transcendentals=0)
    params = pltpu.CompilerParams(vmem_limit_bytes=16 << 20)
    if acc is None:
        return pl.pallas_call(
            first_kernel, in_specs=[VM] * 4, out_specs=VM, compiler_params=params,
            out_shape=jax.ShapeDtypeStruct((n, mu), F32), cost_estimate=cost, name="k_first",
        )(own, par, red, red_par)
    return pl.pallas_call(
        last_kernel, in_specs=[VM] * 5, out_specs=(VM,) * 8, compiler_params=params,
        out_shape=tuple(
            jax.ShapeDtypeStruct((n // 8, mu), F32 if j == 0 else BF) for j in range(8)
        ),
        cost_estimate=cost, name="k_last",
    )(own, par, red, red_par, acc)


def exchange(collocation, density, kernel):
    w = kernel.shape[3]
    gx = lax.axis_index("gx")
    gy = lax.axis_index("gy")
    core, y, xlo = gx & 1, (gx >> 1) & 3, gx >> 3
    z, xhi = gy >> 1, gy & 1
    sign = 1 - 2 * core
    panel = collocation.shape[1]
    mu = density.shape[0]

    own_piece = lax.dynamic_slice_in_dim(collocation, gy * w, w, 1)
    own_t = lax.dot_general(
        collocation, density, (((0,), (1,)), ((), ())), preferred_element_type=F32
    ).astype(BF)

    near = gx_perm(own_piece, YSPLIT)
    other = gx_perm(own_piece, CORE)
    piece_x = gx_perm(own_piece, XLO)
    near_other = gx_perm(other, YSPLIT)
    d_near = both_perm(own_t, ZSPLIT)
    d_other = gx_perm(own_t, CORE)
    d_near_other = both_perm(d_other, ZSPLIT)
    far = gx_perm(near, YSPLIT)
    own_x = gy_perm(own_t, XHI)
    d_far = both_perm(d_near, ZSPLIT)
    px = piece_x
    other_x = gx_perm(px, CORE)
    near_x = gx_perm(px, YSPLIT)
    near_other_x = gx_perm(other_x, YSPLIT)
    dx = own_x
    d_other_x = gx_perm(dx, CORE)
    d_near_x = both_perm(dx, ZSPLIT)
    d_near_other_x = both_perm(d_other_x, ZSPLIT)
    far_x = gx_perm(near_x, YSPLIT)
    d_far_x = both_perm(d_near_x, ZSPLIT)
    pieces = [
        own_piece, other, near, near_other,
        gx_perm(near_other, CORE), gx_perm(near, CORE),
        far, gx_perm(far, CORE),
        piece_x, other_x, near_x, near_other_x,
        gx_perm(near_other_x, CORE), gx_perm(near_x, CORE),
        far_x, gx_perm(far_x, CORE),
    ]
    blocks = [
        own_t, d_near, gx_perm(d_near_other, CORE), d_far,
        own_x, d_near_x, gx_perm(d_near_other_x, CORE), d_far_x,
    ]
    k_tab = []
    for xl in (xlo, 1 - xlo):
        for yy in (y, y - sign, y + sign, y + 2):
            for cc in (core, 1 - core):
                k_tab.append((xl * 4 + (yy & 3)) * 2 + cc)
    m_tab = []
    for h in (xhi, 1 - xhi):
        for zz in (z, z - sign, z + sign, z + 2):
            m_tab.append((zz & 3) * 2 + h)
    m_tab = [m_tab[j] for j in (0, 1, 2, 3, 4, 5, 7, 6)]

    tiles = jnp.transpose(after(kernel, near)[:, :, 0, :], (1, 0, 2))

    hops = [(dx, dy) for dx in (0, 1) for dy in range(4)]
    chips = [((xlo ^ dx) * 4 + ((y + dy) & 3)) * 2 for dx, dy in hops]
    tab = jnp.stack(
        m_tab + k_tab
        + [((z + dz) & 3) * 2 + h for h in (xhi, 1 - xhi) for dz in (2, 1, 3, 0)]
        + [c + 1 - core for c in chips] + [c + core for c in chips]
    ).astype(jnp.int32)
    blocks = [blocks[j] for j in (0, 1, 2, 3, 4, 5, 7, 6)]
    acc = early(tab, blocks[:6], pieces, mu)
    weighted, a1, a2, two_b, x2, one_a, one_b, x1 = weigh(
        tab, acc, tiles, blocks[6:], pieces, mu, 6
    )
    half = panel // 2
    shape = functools.partial(jax.ShapeDtypeStruct, dtype=BF)

    a1 = gy_perm(a1, ZUP)
    a2 = gy_perm(a2, ZDOWN)
    x2 = gy_perm(x2, XHI)
    x1 = gy_perm(x1, XHI)
    three_a, three_b, x3 = spread(tab, weighted, pieces, mu, 2)
    x3 = gy_perm(x3, XHI)
    zero_a, zero_b, x0 = spread(tab, weighted, pieces, mu, 3)
    x0 = gy_perm(x0, XHI)
    b1, b2 = small(pair_kernel, (shape((half // 2, mu)),) * 2, (two_b, x2))
    b1 = gy_perm(b1, ZUP)
    b2 = gy_perm(b2, ZDOWN)

    def merge_a(i, base, got):
        return small(functools.partial(merge_a_kernel, i), shape((half, 2 * mu)), (base, got))

    def merge_b(i, *operands):
        return small(functools.partial(merge_b_kernel, i), shape((half, mu)), operands)

    up_a = gy_perm(merge_a(0, one_a, a1), ZUP)
    down_a = gy_perm(merge_a(1, three_a, a2), ZDOWN)
    up_b = gy_perm(merge_b(0, one_b, x1, b1), ZUP)
    down_b = gy_perm(merge_b(1, three_b, x3, b2), ZDOWN)

    c_own, c_send = pick(tab, after(collocation, far))
    c_par = gx_perm(c_send, CORE)

    sent, kept = small(
        total_a_kernel, (shape((half, mu)), jax.ShapeDtypeStruct((half, mu), F32)),
        (zero_a, up_a, down_a),
    )
    got_x = gy_perm(sent, XHI)
    red_b = small(total_b_kernel, shape((half, mu)), (zero_b, x0, up_b, down_b))
    part = k_rows(c_own, c_par, red_b, gx_perm(red_b, CORE))
    red_a = (kept + got_x.astype(F32)).astype(BF)
    rows = k_rows(c_own, c_par, red_a, gx_perm(red_a, CORE), part)
    total = rows[0]
    for i in (6, 5, 7, 2, 1, 3, 4):
        dx, dy = hops[i]
        pairs = gx_pairs(lambda a, b, c, dx=dx, dy=dy: (a ^ dx, b + dy, c))
        total = total + gx_perm(rows[i], pairs).astype(F32)
    return total


def solution(mesh):
    return jax.shard_map(
        exchange,
        mesh=mesh,
        in_specs=(P(None, "gx"), P("gy", None), P("gx", None, "gy", None)),
        out_specs=P("gx", "gy"),
        check_vma=False,
    )
```

```python
import functools

import jax
import jax.numpy as jnp
from jax import lax
from jax.experimental import pallas as pl
from jax.experimental.pallas import tpu as pltpu
from jax.sharding import PartitionSpec as P


BF = jnp.bfloat16
F32 = jnp.float32
ANY = pl.BlockSpec(memory_space=pl.ANY)
SMEM = pl.BlockSpec(memory_space=pltpu.SMEM)
VM = pl.BlockSpec(memory_space=pltpu.VMEM)
AT_OWN, AT_OTHER, AT_ROWS = 24, 28, 32


def gx_pairs(f):
    out = []
    for a in range(2):
        for b in range(4):
            for c in range(2):
                ta, tb, tc = f(a, b, c)
                out.append(((a * 4 + b) * 2 + c, (ta * 4 + tb % 4) * 2 + tc))
    return out


def gy_pairs(f):
    out = []
    for z in range(4):
        for h in range(2):
            tz, th = f(z, h)
            out.append((z * 2 + h, (tz % 4) * 2 + th))
    return out


def both_pairs(f):
    out = []
    for g in range(16):
        for z in range(4):
            for h in range(2):
                tz, th = f(g % 2, z, h)
                out.append((g * 8 + z * 2 + h, g * 8 + (tz % 4) * 2 + th))
    return out


CORE = gx_pairs(lambda a, b, c: (a, b, 1 - c))
XLO = gx_pairs(lambda a, b, c: (1 - a, b, c))
YSPLIT = gx_pairs(lambda a, b, c: (a, b + 1 if c == 0 else b - 1, c))
ZSPLIT = both_pairs(lambda c, z, h: (z + 1 if c == 0 else z - 1, h))
ZBACK = both_pairs(lambda c, z, h: (z - 1 if c == 0 else z + 1, h))
XHI = gy_pairs(lambda z, h: (z, 1 - h))
ZUP = gy_pairs(lambda z, h: (z + 1, h))
ZDOWN = gy_pairs(lambda z, h: (z - 1, h))


def gx_perm(x, pairs):
    return lax.ppermute(x, "gx", pairs)


def gy_perm(x, pairs):
    return lax.ppermute(x, "gy", pairs)


def both_perm(x, pairs):
    return lax.ppermute(x, ("gx", "gy"), pairs)


def after(x, *others):
    return lax.optimization_barrier((x, *others))[0]


def lanes(ref, first, n, rows=slice(None)):
    return jnp.concatenate([ref[first + i, rows, :] for i in range(n)], axis=1)


def ahead(q, n, limit, fetch):
    for k in range(n, limit):
        pl.when(q + n == k)(functools.partial(fetch, k))


def early_kernel(n_d, n_c, mu, tab, *refs):
    d_refs, c_refs, o_ref = refs[:n_d], refs[n_d : n_d + n_c], refs[n_d + n_c]
    d_s, c_s, o_s, d_sem, c_sem, o_sem = refs[n_d + n_c + 1 :]

    def c_copy(ref, p, j, rows):
        return pltpu.make_async_copy(
            ref.at[pl.ds(rows, mu), :], c_s.at[p, pl.ds(j * mu, mu), :], c_sem.at[p, j]
        )

    def o_copy(q):
        return pltpu.make_async_copy(o_s.at[q], o_ref.at[q], o_sem.at[q])

    def fetch(q):
        for p in range(4 * q, 4 * q + 4):
            for j in range(n_d):
                c_copy(c_refs[p], p, j, pl.multiple_of(tab[j] * mu, mu)).start()

    for j in range(n_d):
        pltpu.make_async_copy(d_refs[j], d_s.at[j], d_sem.at[j]).start()
    fetch(0)
    for j in range(n_d):
        pltpu.make_async_copy(d_refs[j], d_s.at[j], d_sem.at[j]).wait()
    fetch(1)

    def tile(q, carry):
        for i in range(4):
            for j in range(n_d):
                c_copy(c_refs[0], 4 * q + i, j, 0).wait()
        ahead(q, 2, n_c // 4, fetch)
        for h in range(2):
            o_s[2 * q + h] = jnp.dot(
                lanes(d_s, 0, n_d), lanes(c_s, 4 * q + 2 * h, 2), preferred_element_type=F32
            ).astype(BF)
        o_copy(2 * q).start()
        o_copy(2 * q + 1).start()
        return carry

    lax.fori_loop(0, n_c // 4, tile, 0)
    for q in range(n_c // 4):
        o_copy(2 * q).wait()
        o_copy(2 * q + 1).wait()


def early(tab, blocks, pieces, mu):
    n_d, n_c = len(blocks), len(pieces)
    panel = blocks[0].shape[0]
    return pl.pallas_call(
        functools.partial(early_kernel, n_d, n_c, mu),
        out_shape=jax.ShapeDtypeStruct((n_c // 2, panel, 256), BF),
        in_specs=[SMEM] + [ANY] * (n_d + n_c),
        out_specs=ANY,
        scratch_shapes=[
            pltpu.VMEM((n_d, panel, mu), BF),
            pltpu.VMEM((n_c, n_d * mu, 128), BF),
            pltpu.VMEM((n_c // 2, panel, 256), BF),
            pltpu.SemaphoreType.DMA((n_d,)),
            pltpu.SemaphoreType.DMA((n_c, n_d)),
            pltpu.SemaphoreType.DMA((n_c // 2,)),
        ],
        compiler_params=pltpu.CompilerParams(vmem_limit_bytes=60 << 20),
        cost_estimate=pl.CostEstimate(
            flops=2 * panel * n_c * 128 * n_d * mu, bytes_accessed=24 << 20, transcendentals=0
        ),
        name="early",
    )(tab, *blocks, *pieces)


def u_parts(w_ref, c_s, first_row, mu, outs):
    u = lax.dot_general(
        lanes(w_ref, 0, w_ref.shape[0]),
        lanes(c_s, 0, c_s.shape[0], slice(first_row, first_row + 2 * mu)),
        (((1,), (1,)), ((), ())), preferred_element_type=F32,
    ).astype(BF)
    half = u.shape[0] // 2
    a_refs, own_ref, other_ref = outs[:-2], outs[-2], outs[-1]
    rows = half // len(a_refs)
    for i, ref in enumerate(a_refs):
        ref[...] = u[i * rows : (i + 1) * rows]
    own_ref[...] = u[half:, :mu]
    other_ref[...] = u[half:, mu:]


def u_shapes(half, mu, parts):
    a = (jax.ShapeDtypeStruct((half // parts, 2 * mu), BF),) * parts
    return a + (jax.ShapeDtypeStruct((half, mu), BF),) * 2


def weigh_kernel(n_d, n_c, mu, first, tab, *refs):
    acc_ref, z_ref = refs[:2]
    d_refs, c_refs = refs[2 : 2 + n_d], refs[2 + n_d : 2 + n_d + n_c]
    outs = refs[2 + n_d + n_c : 10 + n_d + n_c]
    d_s, c_s, f_s, z_s, w_s, d_sem, c_sem, f_sem, z_sem, a_sem, o_sem = refs[10 + n_d + n_c :]
    tiles = n_c // 2

    def c_copy(ref, p, j, rows):
        return pltpu.make_async_copy(
            ref.at[pl.ds(rows, mu), :], c_s.at[p, pl.ds(j * mu, mu), :], c_sem.at[p, j]
        )

    def z_copy(p, k):
        return pltpu.make_async_copy(z_ref.at[k], z_s.at[p], z_sem.at[p])

    def acc_copy(q):
        return pltpu.make_async_copy(acc_ref.at[q], w_s.at[q], a_sem.at[q])

    def far_copy(p, i):
        place = tab[(AT_OWN, AT_OTHER)[i % 2] + i // 2]
        return pltpu.make_async_copy(
            c_refs[p].at[pl.ds(pl.multiple_of(place * mu, mu), mu), :],
            f_s.at[p, pl.ds(i * mu, mu), :], f_sem.at[p, i],
        )

    def w_copy(q):
        return pltpu.make_async_copy(w_s.at[q], outs[0].at[q], o_sem.at[q])

    def fetch(q):
        for p in (2 * q, 2 * q + 1):
            for j in range(n_d):
                c_copy(c_refs[p], p, j, pl.multiple_of(tab[first + j] * mu, mu)).start()
            z_copy(p, tab[8 + p]).start()
        acc_copy(q).start()

    def fetch_far(q):
        for p in (2 * q, 2 * q + 1):
            for i in range(4):
                far_copy(p, i).start()

    for j in range(n_d):
        pltpu.make_async_copy(d_refs[j], d_s.at[j], d_sem.at[j]).start()
    for q in range(2):
        fetch(q)
    for j in range(n_d):
        pltpu.make_async_copy(d_refs[j], d_s.at[j], d_sem.at[j]).wait()
    fetch(2)

    def tile(q, carry):
        for i in range(2):
            for j in range(n_d):
                c_copy(c_refs[0], 2 * q + i, j, 0).wait()
            z_copy(2 * q + i, 0).wait()
        acc_copy(q).wait()
        ahead(q, 3, tiles, fetch)
        ahead(q, 0, tiles, fetch_far)
        product = jnp.dot(
            lanes(d_s, 0, n_d), lanes(c_s, 2 * q, 2), preferred_element_type=F32
        )
        product = product + w_s[q].astype(F32)
        w_s[q] = (lanes(z_s, 2 * q, 2).astype(F32) * product).astype(BF)
        w_copy(q).start()
        return carry

    lax.fori_loop(0, tiles, tile, 0)
    for p in range(n_c):
        for i in range(4):
            far_copy(p, i).wait()
    u_parts(w_s, f_s, 0, mu, outs[1:5])
    u_parts(w_s, f_s, 2 * mu, mu, outs[5:8])
    for q in range(tiles):
        w_copy(q).wait()


def weigh(tab, acc, tiles, blocks, pieces, mu, first):
    n_d, n_c = len(blocks), len(pieces)
    panel = blocks[0].shape[0]
    half = panel // 2
    return pl.pallas_call(
        functools.partial(weigh_kernel, n_d, n_c, mu, first),
        out_shape=(jax.ShapeDtypeStruct((n_c // 2, panel, 256), BF),)
        + u_shapes(half, mu, 2) + u_shapes(half, mu, 1),
        in_specs=[SMEM] + [ANY] * (n_d + n_c + 2),
        out_specs=(ANY,) + (VM,) * 7,
        scratch_shapes=[
            pltpu.VMEM((n_d, panel, mu), BF),
            pltpu.VMEM((n_c, n_d * mu, 128), BF),
            pltpu.VMEM((n_c, 4 * mu, 128), BF),
            pltpu.VMEM((n_c, panel, 128), BF),
            pltpu.VMEM((n_c // 2, panel, 256), BF),
            pltpu.SemaphoreType.DMA((n_d,)),
            pltpu.SemaphoreType.DMA((n_c, n_d)),
            pltpu.SemaphoreType.DMA((n_c, 4)),
            pltpu.SemaphoreType.DMA((n_c,)),
            pltpu.SemaphoreType.DMA((n_c // 2,)),
            pltpu.SemaphoreType.DMA((n_c // 2,)),
        ],
        compiler_params=pltpu.CompilerParams(vmem_limit_bytes=52 << 20),
        cost_estimate=pl.CostEstimate(
            flops=2 * panel * n_c * 128 * (n_d + 4) * mu, bytes_accessed=24 << 20, transcendentals=0
        ),
        name="weigh",
    )(tab, acc, tiles, *blocks, *pieces)


def spread_kernel(n_c, mu, at, tab, *refs):
    w_ref, c_refs = refs[0], refs[1 : 1 + n_c]
    outs, (w_s, c_s, w_sem, c_sem) = refs[1 + n_c : -4], refs[-4:]

    def c_copy(p, j):
        place = tab[(AT_OWN, AT_OTHER)[j] + at]
        return pltpu.make_async_copy(
            c_refs[p].at[pl.ds(pl.multiple_of(place * mu, mu), mu), :],
            c_s.at[p, pl.ds(j * mu, mu), :], c_sem.at[p, j],
        )

    w_copy = pltpu.make_async_copy(w_ref, w_s, w_sem)
    w_copy.start()
    for p in range(n_c):
        for j in range(2):
            c_copy(p, j).start()
    w_copy.wait()
    for p in range(n_c):
        for j in range(2):
            c_copy(p, j).wait()
    u_parts(w_s, c_s, 0, mu, outs)


def spread(tab, weighted, pieces, mu, at):
    n_c = len(pieces)
    half = weighted.shape[1] // 2
    return pl.pallas_call(
        functools.partial(spread_kernel, n_c, mu, at),
        out_shape=u_shapes(half, mu, 1),
        in_specs=[SMEM] + [ANY] * (n_c + 1),
        out_specs=(VM,) * 3,
        scratch_shapes=[
            pltpu.VMEM(weighted.shape, BF),
            pltpu.VMEM((n_c, 2 * mu, 128), BF),
            pltpu.SemaphoreType.DMA,
            pltpu.SemaphoreType.DMA((n_c, 2)),
        ],
        compiler_params=pltpu.CompilerParams(vmem_limit_bytes=52 << 20),
        cost_estimate=pl.CostEstimate(
            flops=4 * half * n_c * 128 * mu * 2, bytes_accessed=20 << 20, transcendentals=0
        ),
    )(tab, weighted, *pieces)


def small(kernel, out_shape, operands):
    many = isinstance(out_shape, tuple)
    return pl.pallas_call(
        kernel,
        in_specs=[VM] * len(operands),
        out_specs=(VM,) * len(out_shape) if many else VM,
        out_shape=out_shape,
        compiler_params=pltpu.CompilerParams(vmem_limit_bytes=12 << 20),
        cost_estimate=pl.CostEstimate(flops=1 << 26, bytes_accessed=4 << 20, transcendentals=0),
    )(*operands)


def pair_kernel(own_ref, got_ref, up_ref, down_ref):
    rows = up_ref.shape[0]
    for out, part in ((up_ref, slice(0, rows)), (down_ref, slice(rows, 2 * rows))):
        out[...] = (own_ref[part, :].astype(F32) + got_ref[part, :].astype(F32)).astype(BF)


def merge_a_kernel(i, base_ref, got_ref, out_ref):
    rows = got_ref.shape[0]
    there, rest = slice(i * rows, (i + 1) * rows), slice((1 - i) * rows, (2 - i) * rows)
    out_ref[rest, :] = base_ref[rest, :]
    out_ref[there, :] = (base_ref[there, :].astype(F32) + got_ref[...].astype(F32)).astype(BF)


def merge_b_kernel(i, base_ref, x_ref, got_ref, out_ref):
    rows = got_ref.shape[0]
    there, rest = slice(i * rows, (i + 1) * rows), slice((1 - i) * rows, (2 - i) * rows)
    out_ref[rest, :] = (base_ref[rest, :].astype(F32) + x_ref[rest, :].astype(F32)).astype(BF)
    out_ref[there, :] = (
        base_ref[there, :].astype(F32)
        + x_ref[there, :].astype(F32)
        + got_ref[...].astype(F32)
    ).astype(BF)


def total_a_kernel(base_ref, below_ref, above_ref, sent_ref, kept_ref):
    mu = sent_ref.shape[1]
    for out, cols in ((kept_ref, slice(0, mu)), (sent_ref, slice(mu, 2 * mu))):
        out[...] = (
            base_ref[:, cols].astype(F32)
            + below_ref[:, cols].astype(F32)
            + above_ref[:, cols].astype(F32)
        ).astype(out.dtype)


def total_b_kernel(base_ref, x_ref, below_ref, above_ref, out_ref):
    out_ref[...] = (
        base_ref[...].astype(F32)
        + x_ref[...].astype(F32)
        + below_ref[...].astype(F32)
        + above_ref[...].astype(F32)
    ).astype(BF)


def pick_kernel(tab, c_ref, keep_ref, send_ref, buf, in_sem, out_sem):
    n, rows = 8, buf.shape[1] // 8

    def get(i, j):
        start = pl.multiple_of(tab[AT_ROWS + i * n + j] * rows, rows)
        return pltpu.make_async_copy(
            c_ref.at[pl.ds(start, rows), :], buf.at[i, pl.ds(j * rows, rows), :], in_sem.at[i, j]
        )

    for i in range(2):
        for j in range(n):
            get(i, j).start()
    for i, out in ((0, send_ref), (1, keep_ref)):
        for j in range(n):
            get(i, j).wait()
        pltpu.make_async_copy(buf.at[i], out, out_sem.at[i]).start()
    for i, out in ((0, send_ref), (1, keep_ref)):
        pltpu.make_async_copy(buf.at[i], out, out_sem.at[i]).wait()


def pick(tab, collocation):
    nbf, panel = collocation.shape
    block = jax.ShapeDtypeStruct((nbf // 2, panel), BF)
    return pl.pallas_call(
        pick_kernel,
        out_shape=(block, block),
        in_specs=[SMEM, ANY],
        out_specs=(ANY, ANY),
        scratch_shapes=[
            pltpu.VMEM((2, nbf // 2, panel), BF),
            pltpu.SemaphoreType.DMA((2, 8)),
            pltpu.SemaphoreType.DMA((2,)),
        ],
        cost_estimate=pl.CostEstimate(
            flops=1 << 30, bytes_accessed=4 * nbf * panel, transcendentals=0
        ),
        name="pick",
    )(tab, collocation)


def first_kernel(own_ref, par_ref, r_ref, rp_ref, o_ref):
    depth = r_ref.shape[0]
    o_ref[...] = jnp.dot(
        own_ref[:, depth:], r_ref[...], preferred_element_type=F32
    ) + jnp.dot(par_ref[:, depth:], rp_ref[...], preferred_element_type=F32)


def last_kernel(own_ref, par_ref, r_ref, rp_ref, acc_ref, *outs):
    rows, depth = outs[0].shape[0], r_ref.shape[0]
    for j, out in enumerate(outs):
        part = slice(j * rows, (j + 1) * rows)
        out[...] = (
            acc_ref[part, :]
            + jnp.dot(own_ref[part, :depth], r_ref[...], preferred_element_type=F32)
            + jnp.dot(par_ref[part, :depth], rp_ref[...], preferred_element_type=F32)
        ).astype(out.dtype)


def k_rows(own, par, red, red_par, acc=None):
    n, depth = own.shape[0], red.shape[0]
    mu = red.shape[1]
    cost = pl.CostEstimate(flops=4 * n * depth * mu, bytes_accessed=6 << 20, transcendentals=0)
    params = pltpu.CompilerParams(vmem_limit_bytes=16 << 20)
    if acc is None:
        return pl.pallas_call(
            first_kernel, in_specs=[VM] * 4, out_specs=VM, compiler_params=params,
            out_shape=jax.ShapeDtypeStruct((n, mu), F32), cost_estimate=cost, name="k_first",
        )(own, par, red, red_par)
    return pl.pallas_call(
        last_kernel, in_specs=[VM] * 5, out_specs=(VM,) * 8, compiler_params=params,
        out_shape=tuple(
            jax.ShapeDtypeStruct((n // 8, mu), F32 if j == 0 else BF) for j in range(8)
        ),
        cost_estimate=cost, name="k_last",
    )(own, par, red, red_par, acc)


def exchange(collocation, density, kernel):
    w = kernel.shape[3]
    gx = lax.axis_index("gx")
    gy = lax.axis_index("gy")
    core, y, xlo = gx & 1, (gx >> 1) & 3, gx >> 3
    z, xhi = gy >> 1, gy & 1
    sign = 1 - 2 * core
    panel = collocation.shape[1]
    mu = density.shape[0]

    own_piece = lax.dynamic_slice_in_dim(collocation, gy * w, w, 1)
    own_t = lax.dot_general(
        collocation, density, (((0,), (1,)), ((), ())), preferred_element_type=F32
    ).astype(BF)

    near = gx_perm(own_piece, YSPLIT)
    other = gx_perm(own_piece, CORE)
    piece_x = gx_perm(own_piece, XLO)
    near_other = gx_perm(other, YSPLIT)
    d_near = both_perm(own_t, ZSPLIT)
    d_back = both_perm(own_t, ZBACK)
    far = gx_perm(near, YSPLIT)
    own_x = gy_perm(own_t, XHI)
    d_far = both_perm(d_near, ZSPLIT)
    px = piece_x
    other_x = gx_perm(px, CORE)
    near_x = gx_perm(px, YSPLIT)
    near_other_x = gx_perm(other_x, YSPLIT)
    dx = own_x
    d_near_x = both_perm(dx, ZSPLIT)
    d_back_x = both_perm(dx, ZBACK)
    far_x = gx_perm(near_x, YSPLIT)
    d_far_x = both_perm(d_near_x, ZSPLIT)
    pieces = [
        own_piece, other, near, near_other,
        gx_perm(near_other, CORE), gx_perm(near, CORE),
        far, gx_perm(far, CORE),
        piece_x, other_x, near_x, near_other_x,
        gx_perm(near_other_x, CORE), gx_perm(near_x, CORE),
        far_x, gx_perm(far_x, CORE),
    ]
    blocks = [
        own_t, d_near, d_back, d_far,
        own_x, d_near_x, d_back_x, d_far_x,
    ]
    k_tab = []
    for xl in (xlo, 1 - xlo):
        for yy in (y, y - sign, y + sign, y + 2):
            for cc in (core, 1 - core):
                k_tab.append((xl * 4 + (yy & 3)) * 2 + cc)
    m_tab = []
    for h in (xhi, 1 - xhi):
        for zz in (z, z - sign, z + sign, z + 2):
            m_tab.append((zz & 3) * 2 + h)
    m_tab = [m_tab[j] for j in (0, 1, 2, 3, 4, 5, 7, 6)]

    tiles = jnp.transpose(after(kernel, near)[:, :, 0, :], (1, 0, 2))

    hops = [(dx, dy) for dx in (0, 1) for dy in range(4)]
    chips = [((xlo ^ dx) * 4 + ((y + dy) & 3)) * 2 for dx, dy in hops]
    tab = jnp.stack(
        m_tab + k_tab
        + [((z + dz) & 3) * 2 + h for h in (xhi, 1 - xhi) for dz in (2, 1, 3, 0)]
        + [c + 1 - core for c in chips] + [c + core for c in chips]
    ).astype(jnp.int32)
    blocks = [blocks[j] for j in (0, 1, 2, 3, 4, 5, 7, 6)]
    acc = early(tab, blocks[:6], pieces, mu)
    weighted, a1, a2, two_b, x2, one_a, one_b, x1 = weigh(
        tab, acc, tiles, blocks[6:], pieces, mu, 6
    )
    half = panel // 2
    shape = functools.partial(jax.ShapeDtypeStruct, dtype=BF)

    a1 = gy_perm(a1, ZUP)
    a2 = gy_perm(a2, ZDOWN)
    x2 = gy_perm(x2, XHI)
    x1 = gy_perm(x1, XHI)
    three_a, three_b, x3 = spread(tab, weighted, pieces, mu, 2)
    x3 = gy_perm(x3, XHI)
    zero_a, zero_b, x0 = spread(tab, weighted, pieces, mu, 3)
    x0 = gy_perm(x0, XHI)
    b1, b2 = small(pair_kernel, (shape((half // 2, mu)),) * 2, (two_b, x2))
    b1 = gy_perm(b1, ZUP)
    b2 = gy_perm(b2, ZDOWN)

    def merge_a(i, base, got):
        return small(functools.partial(merge_a_kernel, i), shape((half, 2 * mu)), (base, got))

    def merge_b(i, *operands):
        return small(functools.partial(merge_b_kernel, i), shape((half, mu)), operands)

    up_a = gy_perm(merge_a(0, one_a, a1), ZUP)
    down_a = gy_perm(merge_a(1, three_a, a2), ZDOWN)
    up_b = gy_perm(merge_b(0, one_b, x1, b1), ZUP)
    down_b = gy_perm(merge_b(1, three_b, x3, b2), ZDOWN)

    c_own, c_send = pick(tab, after(collocation, far))
    c_par = gx_perm(c_send, CORE)

    sent, kept = small(
        total_a_kernel, (shape((half, mu)), jax.ShapeDtypeStruct((half, mu), F32)),
        (zero_a, up_a, down_a),
    )
    got_x = gy_perm(sent, XHI)
    red_b = small(total_b_kernel, shape((half, mu)), (zero_b, x0, up_b, down_b))
    part = k_rows(c_own, c_par, red_b, gx_perm(red_b, CORE))
    red_a = (kept + got_x.astype(F32)).astype(BF)
    rows = k_rows(c_own, c_par, red_a, gx_perm(red_a, CORE), part)
    total = rows[0]
    for i in (6, 5, 7, 2, 1, 3, 4):
        dx, dy = hops[i]
        pairs = gx_pairs(lambda a, b, c, dx=dx, dy=dy: (a ^ dx, b + dy, c))
        total = total + gx_perm(rows[i], pairs).astype(F32)
    return total


def solution(mesh):
    return jax.shard_map(
        exchange,
        mesh=mesh,
        in_specs=(P(None, "gx"), P("gy", None), P("gx", None, "gy", None)),
        out_specs=P("gx", "gy"),
        check_vma=False,
    )
```
